16 devices in a mesh: dp: 2 (over y, z), tp: 8 (over x, core).
Axes of the slice: x: 4, y: 2, z: 1, core: 2. Of those that a mesh axis runs over, the one named last changes fastest.
The devices are a block of a 4x4x8 slice.
Arguments:
- x: bfloat16 [4096, 7168], P(('dp', 'tp')), parts along dimension 0
- gain_a: bfloat16 [7168], replicated
- wq: bfloat16 [7168, 7168], P(None, 'tp')
- wk: bfloat16 [7168, 1024], P(None, 'tp')
- wv: bfloat16 [7168, 1024], P(None, 'tp')
- wo: bfloat16 [7168, 7168], P('tp')
- gain_m: bfloat16 [7168], replicated
- w_gate: bfloat16 [7168, 20480], P(None, 'tp')
- w_up: bfloat16 [7168, 20480], P(None, 'tp')
- w_down: bfloat16 [20480, 7168], P('tp')
Outputs:
- output: bfloat16 [4096, 7168], P(('dp', 'tp')), parts along dimension 0
There are 2 independent parts. The reference program is written for one: setup_inputs(seed, part) draws one part's arguments, and reference() takes and returns one part's arrays. A program takes and returns all parts, laid end to end along the dimension named above; an argument that names none is the same for every part.
All inputs are finite; a program needn't handle non-finite values.
Results may differ from the reference program's by a relative error of at most 0.017.
Values are sent between devices in bfloat16 or wider.
A program may use at most 768 MiB of HBM per device.

```python
import jax
import jax.numpy as jnp
from jax import lax

ROWS = 2048
D = 7168
HEADS = 56
KV_HEADS = 8
HEAD = 128
FF = 20480
THETA = 10000


def setup_inputs(seed: int = 0, part: int = 0) -> dict:
    kx, kn, kq, kk, kv, ko, km, kg, ku, kd = jax.random.split(jax.random.key(seed), 10)

    def weights(key, rows, columns):
        return jax.random.normal(key, (rows, columns), jnp.float32) * rows**-0.5

    drawn = {
        "x": jax.random.normal(jax.random.fold_in(kx, part), (ROWS, D), jnp.float32),
        "gain_a": 1 + 0.1 * jax.random.normal(kn, (D,), jnp.float32),
        "wq": 2 * weights(kq, D, HEADS * HEAD),
        "wk": 2 * weights(kk, D, KV_HEADS * HEAD),
        "wv": 4 * weights(kv, D, KV_HEADS * HEAD),
        "wo": weights(ko, HEADS * HEAD, D),
        "gain_m": 1 + 0.1 * jax.random.normal(km, (D,), jnp.float32),
        "w_gate": weights(kg, D, FF),
        "w_up": weights(ku, D, FF),
        "w_down": 2 * weights(kd, FF, D),
    }
    return {k: v.astype(jnp.bfloat16) for k, v in drawn.items()}


def normed(x, gain):
    wide = x.astype(jnp.float32)
    scale = lax.rsqrt(jnp.mean(wide * wide, -1, keepdims=True) + 1e-6)
    return (wide * scale * gain.astype(jnp.float32)).astype(jnp.bfloat16)


def turned(t, place, theta):
    half = t.shape[-1] // 2
    angle = place.astype(jnp.float32)[:, None] * theta ** (-jnp.arange(half, dtype=jnp.float32) / half)
    cos, sin = jnp.cos(angle)[:, None], jnp.sin(angle)[:, None]
    a, b = t[..., :half].astype(jnp.float32), t[..., half:].astype(jnp.float32)
    return jnp.concatenate([a * cos - b * sin, b * cos + a * sin], -1).astype(jnp.bfloat16)


def matmul(a, w):
    return jnp.dot(a, w, preferred_element_type=jnp.float32).astype(jnp.bfloat16)


def einsum(form, a, b):
    return jnp.einsum(form, a.astype(jnp.float32), b.astype(jnp.float32))


def attention(q, k, v):
    scores = einsum("tgsd,ugd->gstu", q, k) * q.shape[-1] ** -0.5
    token = jnp.arange(q.shape[0])
    scores = jnp.where(token[:, None] >= token, scores, -jnp.inf)
    weights = jax.nn.softmax(scores, -1).astype(jnp.bfloat16)
    return einsum("gstu,ugd->tgsd", weights, v).astype(jnp.bfloat16)


def reference(x, gain_a, wq, wk, wv, wo, gain_m, w_gate, w_up, w_down):
    a, place = normed(x, gain_a), jnp.arange(ROWS)
    q = turned(matmul(a, wq).reshape(ROWS, HEADS, HEAD), place, THETA).reshape(ROWS, KV_HEADS, -1, HEAD)
    k = turned(matmul(a, wk).reshape(ROWS, KV_HEADS, HEAD), place, THETA)
    v = matmul(a, wv).reshape(ROWS, KV_HEADS, HEAD)
    seen = attention(q, k, v).reshape(ROWS, HEADS * HEAD)
    h = (x.astype(jnp.float32) + jnp.dot(seen, wo, preferred_element_type=jnp.float32)).astype(jnp.bfloat16)
    b = normed(h, gain_m)
    gate = jnp.dot(b, w_gate, preferred_element_type=jnp.float32)
    up = jnp.dot(b, w_up, preferred_element_type=jnp.float32)
    hidden = (jax.nn.silu(gate) * up).astype(jnp.bfloat16)
    return (h.astype(jnp.float32) + jnp.dot(hidden, w_down, preferred_element_type=jnp.float32)).astype(jnp.bfloat16)
```

```python
import functools

import jax
import jax.numpy as jnp
from jax import lax
from jax.experimental import pallas as pl
from jax.experimental.pallas import tpu as pltpu


from jax.sharding import PartitionSpec as P

VMEM = 56 * 2**20
MOST = 67_043_328
HIDDEN = -1e30
LOG2E = 1.4426950408889634
KEYS = 512

HEAD = 128
THETA = 10000
MESH = pl.DeviceIdType.MESH
CHIPS = 4
LO, HI = 0, 1
WAVES = (((0, LO), (0, HI)), ((-1, LO), (1, HI)), ((2, LO), (2, HI)), ((-1, HI), (1, LO)))
RING = (WAVES[1] + WAVES[3] + WAVES[2])
ACROSS = WAVES[0] + RING
GU = 256
TN = 512
ANY = pl.BlockSpec(memory_space=pl.ANY)
WHOLE = pl.BlockSpec(memory_space=pltpu.VMEM)


def normed(x, gain):
    wide = x.astype(jnp.float32)
    scale = lax.rsqrt(jnp.mean(wide * wide, -1, keepdims=True) + 1e-6)
    return (wide * scale * gain.astype(jnp.float32)).astype(jnp.bfloat16)


def turns(rows, fine, theta):
    half = HEAD // 2

    def both(places):
        angle = places.astype(jnp.float32)[:, None] * theta ** (-jnp.arange(half, dtype=jnp.float32) / half)
        return jnp.cos(angle), jnp.sin(angle)

    cos, sin = both(jnp.arange(rows // fine) * fine)
    coarse = jnp.stack([jnp.concatenate([cos, cos], -1), jnp.concatenate([sin, sin], -1)], 1)
    cos, sin = both(jnp.arange(fine))
    return coarse, jnp.stack([jnp.concatenate(t, -1) for t in ((cos, cos), (sin, sin), (-cos, cos), (-sin, sin))])


class Place:
    def __init__(self):
        me = lax.axis_index("tp")
        self.me, self.chip, self.core = me, lax.div(me, 2), lax.rem(me, 2)
        self.next, self.previous, self.other = self.device(1), self.device(-1), self.device(0, True)

    def device(self, away, across=False):
        return lax.rem(self.chip + (away + CHIPS), CHIPS) * 2 + (1 - self.core if across else self.core)

    def hello(self):
        for d in (self.next, self.previous, self.other):
            pl.semaphore_signal(pltpu.get_barrier_semaphore(), inc=1, device_id={"tp": d}, device_id_type=MESH)

    def meet(self):
        pl.semaphore_wait(pltpu.get_barrier_semaphore(), 3)


def remote(src, dst, send, recv, to):
    return pltpu.make_async_remote_copy(src_ref=src, dst_ref=dst, send_sem=send, recv_sem=recv, device_id={"tp": to}, device_id_type=MESH)


class Gather:
    def __init__(self, place, own, all_, send, recv, land=None):
        self.place, self.own, self.all, self.send, self.recv, self.land = place, own, all_, send, recv, land

    def to_next(self, half):
        i = RING.index((-1, half))
        return remote(self.own.at[half], self.all.at[self.place.me, half], self.send.at[half], self.recv.at[i], self.place.next)

    def to_previous(self, half):
        i = RING.index((1, half))
        return remote(self.own.at[half], self.all.at[self.place.me, half], self.send.at[2 + half], self.recv.at[i], self.place.previous)

    def onward(self, half):
        ref = self.all.at[self.place.device(-1 if half == LO else 1), half]
        to = self.place.next if half == LO else self.place.previous
        return remote(ref, ref, self.send.at[4 + half], self.recv.at[RING.index((2, half))], to)

    def across(self, piece):
        i = 6 + ACROSS.index(piece)
        away, half = piece
        dst = self.all.at[self.place.device(away), half]
        src = self.own.at[half] if away == 0 else dst
        return remote(src, self.land(piece) if self.land else dst, self.send.at[i], self.recv.at[i], self.place.other)

    def arrive(self, piece, across=False):
        away, half = piece
        ref = self.land(piece) if across and self.land else self.all.at[self.place.device(away, across), half]
        i = 6 + ACROSS.index(piece) if across else RING.index(piece)
        remote(ref, ref, self.send.at[i], self.recv.at[i], self.place.other).wait_recv()

    def piece(self, piece, across=False):
        away, half = piece
        return self.own.at[half] if away == 0 and not across else self.all.at[self.place.device(away, across), half]

    def drain(self, pieces):
        for half in (LO, HI):
            self.to_next(half).wait_send()
            self.to_previous(half).wait_send()
            if (2, half) in pieces:
                self.onward(half).wait_send()
        for piece in pieces:
            self.across(piece).wait_send()


def normalize(ref, to, first, count, gain_ref):
    many = 32

    def some(i, _):
        here = pl.ds(pl.multiple_of(first + i * many, many), many)
        to[here, :] = normed(ref[here, :], gain_ref[...])

    lax.fori_loop(0, count // many, some, None)


def gather_qkv(x, gain, wq, wk, wv, coarse, fine):
    both, d = x.shape
    half, quarter = both // 2, both // 4
    n = CHIPS * 2
    rows, heads = n * both, wq.shape[1] // HEAD
    order = (0, 1, 3, 2)

    def kernel(x_ref, gain_ref, wq_ref, wk_ref, wv_ref, coarse_ref, fine_ref, q_ref, k_ref, v_ref, all_ref, own_ref,
               w, xs, st, send, recv, psend, precv, wsem, xsem, osem):
        place = Place()
        place.hello()
        quarters = [pl.ds(i * quarter, quarter) for i in range(4)]
        given = [pltpu.make_async_copy(x_ref.at[quarters[i]], xs.at[quarters[i]], xsem.at[i]) for i in range(4)]
        kept = [pltpu.make_async_copy(xs.at[quarters[i]], own_ref.at[i // 2, i % 2], xsem.at[i]) for i in range(4)]
        loads = [
            pltpu.make_async_copy(wq_ref, w.at[:, pl.ds(0, heads * HEAD)], wsem.at[0]),
            pltpu.make_async_copy(wk_ref, w.at[:, pl.ds(heads * HEAD, HEAD)], wsem.at[1]),
            pltpu.make_async_copy(wv_ref, w.at[:, pl.ds((heads + 1) * HEAD, HEAD)], wsem.at[2]),
        ]
        for c in given:
            c.start()
        for i in range(4):
            given[i].wait()
            normalize(xs, xs, i * quarter, quarter, gain_ref)
            kept[i].start()
        place.meet()
        g = Gather(place, own_ref, all_ref, send, recv)
        for c in kept:
            c.wait()
        g.to_next(LO).start()
        g.to_previous(HI).start()
        for piece in WAVES[0]:
            g.across(piece).start()
        g.to_next(HI).start()
        g.to_previous(LO).start()
        for c in loads:
            c.start()
        for c in loads:
            c.wait()

        def parts(v):
            if v < 6:
                return [(p, v % 2 == 1, i) for p in WAVES[order[v // 2]] for i in (0, 1)]
            return [(p, across, v - 6) for across in (False, True) for p in WAVES[2]]

        def block(v, i):
            at = 0
            for s in range(8):
                (away, h), across, e = parts(s)[i]
                at = jnp.where(v == s, place.device(away, across) * 4 + h * 2 + e, at)
            return at

        def opposite(h, e, across):
            ref = all_ref.at[place.device(2), h, e]
            if across:
                return remote(ref, ref, psend.at[1, h, e], precv.at[1, h, e], place.other)
            ref = all_ref.at[place.device(-1 if h == LO else 1), h, e]
            return remote(ref, ref, psend.at[0, h, e], precv.at[0, h, e], place.next if h == LO else place.previous)

        def reached(h, e, across):
            ref = all_ref.at[place.device(2, across), h, e]
            k = 1 if across else 0
            remote(ref, ref, psend.at[k, h, e], precv.at[k, h, e], place.other).wait_recv()

        def outs(slot, v):
            r = []
            for i in range(4):
                here = quarters[i]
                to = pl.ds(pl.multiple_of(block(v, i) * quarter, quarter), quarter)
                r.append(pltpu.make_async_copy(st.at[slot, pl.ds(0, heads), here], q_ref.at[:, to], osem.at[slot, i, 0]))
                r.append(pltpu.make_async_copy(st.at[slot, heads, here], k_ref.at[0, to], osem.at[slot, i, 1]))
                r.append(pltpu.make_async_copy(st.at[slot, heads + 1, here], v_ref.at[0, to], osem.at[slot, i, 2]))
            return r

        def fetch(v, which):
            copies = []
            for i in which:
                piece, across, e = parts(v)[i]
                copies.append(pltpu.make_async_copy(g.piece(piece, across).at[e], xs.at[quarters[i]], xsem.at[i]))
            for c in copies:
                c.start()
            return copies

        def ready(v):
            wave = order[v // 2]
            if v >= 6:
                for h in (LO, HI):
                    reached(h, v - 6, False)
                    opposite(h, v - 6, True).start()
                copies = fetch(v, (0, 1))
                for h in (LO, HI):
                    reached(h, v - 6, True)
                copies += fetch(v, (2, 3))
            else:
                for p in WAVES[wave]:
                    g.arrive(p, v % 2 == 1)
                if v == 2:
                    for e in (0, 1):
                        for h in (LO, HI):
                            opposite(h, e, False).start()
                if v % 2 == 0:
                    for p in WAVES[wave]:
                        g.across(p).start()
                copies = fetch(v, range(4))
            for c in copies:
                c.wait()

        def step(v, _):
            for s in range(1, 8):
                pl.when(v == s)(functools.partial(ready, s))

            slot = lax.rem(v, 2)

            @pl.when(v >= 2)
            def _():
                for c in outs(slot, v - 2):
                    c.wait()

            def chunk(j, _):
                at = pl.multiple_of(j * 2 * HEAD, 2 * HEAD)
                t = jnp.dot(xs[...], w[:, pl.ds(at, 2 * HEAD)], preferred_element_type=jnp.float32).astype(jnp.bfloat16).astype(jnp.float32)
                for i in range(4):
                    a = coarse_ref[block(v, i)]
                    cos = a[:1] * fine_ref[0] - a[1:] * fine_ref[1]
                    sin = a[1:] * fine_ref[2] + a[:1] * fine_ref[3]
                    for e in (0, 1):
                        u = t[i * quarter : (i + 1) * quarter, e * HEAD : (e + 1) * HEAD]
                        st[slot, 2 * j + e, i * quarter : (i + 1) * quarter, :] = (u * cos + pltpu.roll(u, HEAD // 2, 1) * sin).astype(jnp.bfloat16)

            lax.fori_loop(0, (heads + 1) // 2, chunk, None)
            st[slot, heads + 1] = jnp.dot(xs[...], w[:, (heads + 1) * HEAD :], preferred_element_type=jnp.float32).astype(jnp.bfloat16)
            for c in outs(slot, v):
                c.start()

        lax.fori_loop(0, 2 * CHIPS, step, None)
        for slot in (0, 1):
            for c in outs(slot, 2 * CHIPS - 2 + slot):
                c.wait()
        g.drain(WAVES[0] + WAVES[1] + WAVES[3])
        for h in (LO, HI):
            for e in (0, 1):
                opposite(h, e, False).wait_send()
                opposite(h, e, True).wait_send()

    return pl.pallas_call(
        kernel,
        out_shape=[
            jax.ShapeDtypeStruct((heads, rows, HEAD), jnp.bfloat16),
            jax.ShapeDtypeStruct((1, rows, HEAD), jnp.bfloat16),
            jax.ShapeDtypeStruct((1, rows, HEAD), jnp.bfloat16),
            jax.ShapeDtypeStruct((n, 2, 2, quarter, d), jnp.bfloat16),
            jax.ShapeDtypeStruct((2, 2, quarter, d), jnp.bfloat16),
        ],
        in_specs=[ANY, WHOLE, ANY, ANY, ANY, WHOLE, WHOLE],
        out_specs=[ANY] * 5,
        scratch_shapes=[
            pltpu.VMEM((d, (heads + 2) * HEAD), jnp.bfloat16),
            pltpu.VMEM((both, d), jnp.bfloat16),
            pltpu.VMEM((2, heads + 2, both, HEAD), jnp.bfloat16),
            pltpu.SemaphoreType.DMA((14,)),
            pltpu.SemaphoreType.DMA((14,)),
            pltpu.SemaphoreType.DMA((2, 2, 2)),
            pltpu.SemaphoreType.DMA((2, 2, 2)),
            pltpu.SemaphoreType.DMA((3,)),
            pltpu.SemaphoreType.DMA((4,)),
            pltpu.SemaphoreType.DMA((2, 4, 3)),
        ],
        compiler_params=pltpu.CompilerParams(collective_id=0, has_side_effects=True, vmem_limit_bytes=VMEM),
        cost_estimate=pl.CostEstimate(flops=2 * rows * d * (heads + 2) * HEAD, bytes_accessed=2 * rows * d * 2, transcendentals=0),
        name="gather_qkv",
    )(x, gain, wq, wk, wv, coarse, fine)[:3]


class Scatter:
    def __init__(self, place, hid, right, out, wd, sent, came, mine, passed, wsem, asend, arecv, ssem, rsem, clear):
        self.place, self.hid, self.right, self.wd, self.sent, self.came, self.mine, self.out, self.passed = (
            place, hid, right, wd, sent, came, mine, out, passed)
        self.wsem, self.asend, self.arecv, self.ssem, self.rsem, self.clear = wsem, asend, arecv, ssem, rsem, clear
        self.tiles = right.shape[1] // TN
        self.half = sent.shape[1] // 2

    @staticmethod
    def scratch(half, k, d):
        tiles = d // TN
        return [
            pltpu.VMEM((3, k, TN), jnp.bfloat16),
            pltpu.VMEM((2, 2 * half, TN), jnp.bfloat16),
            pltpu.VMEM((4, 2 * half, TN), jnp.bfloat16),
            pltpu.VMEM((2, 2 * half, TN), jnp.float32),
            pltpu.VMEM((2, 2, tiles, half, TN), jnp.bfloat16),
            pltpu.SemaphoreType.DMA((3,)),
            pltpu.SemaphoreType.DMA((2,)),
            pltpu.SemaphoreType.DMA((4,)),
            pltpu.SemaphoreType.DMA((2, tiles)),
            pltpu.SemaphoreType.DMA((3, 2, tiles)),
            pltpu.SemaphoreType.REGULAR((2,)),
        ]

    def load(self, t):
        at = pl.multiple_of(lax.rem(t, self.tiles) * TN, TN)
        slot = lax.rem(t, 3)
        return pltpu.make_async_copy(self.right.at[:, pl.ds(at, TN)], self.wd.at[slot], self.wsem.at[slot])

    def swap(self, t):
        two, four = lax.rem(t, 2), lax.rem(t, 4)
        return remote(self.sent.at[two], self.came.at[four], self.asend.at[two], self.arecv.at[four], self.place.other)

    def leaving(self, side, t):
        return pl.ds(side * self.half, self.half), pl.ds(pl.multiple_of(t * TN, TN), TN)

    def passing(self, k, side, t):
        to = self.place.previous if side == 0 else self.place.next
        return remote(self.out.at[self.leaving(side, t)], self.passed.at[k % 2, side, t], self.ssem.at[side, t], self.rsem.at[k, side, t], to)

    def wave(self, turn, wave, final=None):
        half, tiles = self.half, self.tiles
        base = turn * tiles

        def finish(t):
            g = base + t
            self.swap(g).wait_recv()
            sums = self.mine[lax.rem(g, 2)] + self.came[lax.rem(g, 4)].astype(jnp.float32)
            parts = [sums[:half], sums[half:]]
            if wave == 1:
                for side in (0, 1):
                    self.passing(0, side, t).wait_recv()
                    parts[side] += self.passed[0, side, t].astype(jnp.float32)
            if final is not None:
                for side in (0, 1):
                    self.passing(1, side, t).wait_recv()
                    self.passing(2, 1 - side, t).wait_recv()
                    parts[side] += self.passed[1, side, t].astype(jnp.float32) + self.passed[0, 1 - side, t].astype(jnp.float32)
                final(t, parts)
                return
            for side in (0, 1):
                if turn > 0:
                    self.passing(turn - 1, side, t).wait_send()
                self.out[self.leaving(side, t)] = parts[side].astype(jnp.bfloat16)
                self.passing(turn, side, t).start()

        def step(t, _):
            g = base + t
            slot = lax.rem(g, 3)
            self.load(g).wait()

            @pl.when(g < 4 * tiles - 2)
            def _():
                self.load(g + 2).start()

            def free():
                self.swap(g - 2).wait_send()

            if turn > 0:
                free()
            else:
                pl.when(t >= 2)(free)
            terms = jnp.dot(self.hid[wave], self.wd[slot], preferred_element_type=jnp.float32)

            self.mine[lax.rem(g, 2)] = terms[: 2 * half]
            self.sent[lax.rem(g, 2)] = terms[2 * half :].astype(jnp.bfloat16)
            self.swap(g).start()

            @pl.when(t > 0)
            def _():
                finish(t - 1)

        if turn == 2:
            for side in (0, 1):
                pl.semaphore_wait(self.clear.at[side], 1)
        lax.fori_loop(0, tiles, step, None)
        finish(tiles - 1)
        if turn == 1:
            for side, to in ((0, self.place.next), (1, self.place.previous)):
                pl.semaphore_signal(self.clear.at[side], inc=1, device_id={"tp": to}, device_id_type=MESH)

    def drain(self):
        for i in (2, 1):
            self.swap(4 * self.tiles - i).wait_send()

        def one(t, _):
            for side in (0, 1):
                self.passing(2, side, t).wait_send()

        lax.fori_loop(0, self.tiles, one, None)


def scatter_out(q, k, v, wo, x, gain):
    (heads, rows, _), (both, d) = q.shape, x.shape
    half, width, block = both // 2, wo.shape[0], min(KEYS, rows)
    cols = heads * half
    strips = ((0, 4 * HEAD), (4 * HEAD, cols))
    scale = HEAD**-0.5 * LOG2E

    def dot(a, b, ca, cb):
        return lax.dot_general(a, b, (((ca,), (cb,)), ((), ())), preferred_element_type=jnp.float32)

    def kernel(q_ref, k_ref, v_ref, wo_ref, x_ref, gain_ref, h_ref, b_ref, hid, xs, bs, leave, qs, ks, vs, vt, top, mix, gap, *rest):
        *rest, qsem, ksem, xsem, osem = rest
        place = Place()
        place.hello()
        s = Scatter(place, hid, wo_ref, leave, *rest)

        def token(wave, p):
            away, h = WAVES[wave][p % 2]
            return pl.multiple_of(place.device(away, p >= 2) * both + h * half, half)

        def queries(wave, p):
            return pltpu.make_async_copy(q_ref.at[:, pl.ds(token(wave, p), half)], qs.at[wave, p], qsem.at[wave, p])

        kv = [pltpu.make_async_copy(k_ref.at[0], ks, ksem.at[0]), pltpu.make_async_copy(v_ref.at[0], vs, ksem.at[1])]
        for c in kv:
            c.start()
        for wave in (2, 1, 3, 0):
            for p in range(4):
                queries(wave, p).start()
        residual = pltpu.make_async_copy(x_ref, xs, xsem)
        residual.start()
        s.load(0).start()
        s.load(1).start()
        gap[...] = lax.broadcasted_iota(jnp.int32, gap.shape, 0) - lax.rem(lax.broadcasted_iota(jnp.int32, gap.shape, 1), half)
        for c in kv:
            c.wait()
        for i in range(rows // block):
            here = slice(i * block, (i + 1) * block)
            vt[:HEAD, here] = vs[here, :].T
        vt[HEAD:, :] = jnp.ones((16, rows), jnp.bfloat16)
        place.meet()

        def attention(wave):
            def piece(p, _):
                first = 0
                for i in range(4):
                    first = jnp.where(p == i, token(wave, i), first)
                top[...] = jnp.full(top.shape, HIDDEN, jnp.float32)
                mix[...] = jnp.zeros(mix.shape, jnp.float32)

                def some(j, masked):
                    here = pl.ds(pl.multiple_of(j * block, block), block)
                    mine = qs[wave, p].reshape(cols, HEAD)
                    scores = [dot(ks[here, :], mine[a:z, :], 1, 1) for a, z in strips]
                    weights, keeps = [], []
                    for (a, z), t in zip(strips, scores):
                        if masked:
                            t = jnp.where(gap[:, a:z] <= first - j * block, t, 2 * HIDDEN)
                        old = top[:, a:z]
                        new = jnp.maximum(old, t.max(axis=0, keepdims=True))
                        top[:, a:z] = new
                        weights.append(jnp.exp2((t - new) * scale).astype(jnp.bfloat16))
                        keeps.append(jnp.exp2((old - new) * scale))
                    for (a, z), t, keep in zip(strips, weights, keeps):
                        mix[:, a:z] = mix[:, a:z] * keep + dot(vt[:, here], t, 1, 0)

                last = lax.div(first, block)
                lax.fori_loop(0, last, lambda j, _: some(j, False), None)
                some(last, True)
                done = (mix[:HEAD, :] * (1 / mix[HEAD : HEAD + 1, :])).T.astype(jnp.bfloat16)
                at = pl.ds(pl.multiple_of(p * half, half), half)
                for i in range(heads):
                    hid[wave, at, i * HEAD : (i + 1) * HEAD] = done[i * half : (i + 1) * half, :]

            for p in range(4):
                queries(wave, p).wait()
            lax.fori_loop(0, 4, piece, None)

        def final(t, parts):
            at = pl.ds(pl.multiple_of(t * TN, TN), TN)
            for side in (0, 1):
                here = pl.ds(side * half, half)
                xs[here, at] = (xs[here, at].astype(jnp.float32) + parts[side]).astype(jnp.bfloat16)

        attention(2)
        s.wave(0, 2)
        attention(1)
        attention(3)
        s.wave(1, 1)
        attention(0)
        s.wave(2, 3)
        residual.wait()
        s.wave(3, 0, final)
        keep = pltpu.make_async_copy(xs, h_ref, xsem)
        keep.start()
        give = [pltpu.make_async_copy(bs.at[pl.ds(i * half, half)], b_ref.at[i], osem.at[i]) for i in (0, 1)]
        for i in (0, 1):
            normalize(xs, bs, i * half, half, gain_ref)
            give[i].start()
        for c in (keep, *give):
            c.wait()
        s.drain()

    return pl.pallas_call(
        kernel,
        out_shape=[jax.ShapeDtypeStruct((both, d), jnp.bfloat16), jax.ShapeDtypeStruct((2, half, d), jnp.bfloat16)],
        in_specs=[ANY] * 5 + [WHOLE],
        out_specs=[ANY] * 2,
        scratch_shapes=[
            pltpu.VMEM((4, 4 * half, width), jnp.bfloat16),
            pltpu.VMEM((both, d), jnp.bfloat16),
            pltpu.VMEM((both, d), jnp.bfloat16),
            pltpu.VMEM((both, d), jnp.bfloat16),
            pltpu.VMEM((4, 4, heads, half, HEAD), jnp.bfloat16),
            pltpu.VMEM((rows, HEAD), jnp.bfloat16),
            pltpu.VMEM((rows, HEAD), jnp.bfloat16),
            pltpu.VMEM((HEAD + 16, rows), jnp.bfloat16),
            pltpu.VMEM((1, cols), jnp.float32),
            pltpu.VMEM((HEAD + 16, cols), jnp.float32),
            pltpu.VMEM((block, cols), jnp.int32),
            *Scatter.scratch(half, width, d),
            pltpu.SemaphoreType.DMA((4, 4)),
            pltpu.SemaphoreType.DMA((2,)),
            pltpu.SemaphoreType.DMA,
            pltpu.SemaphoreType.DMA((2,)),
        ],
        compiler_params=pltpu.CompilerParams(collective_id=1, has_side_effects=True, vmem_limit_bytes=VMEM),
        cost_estimate=pl.CostEstimate(flops=2 * rows * d * width, bytes_accessed=8 * d * width, transcendentals=heads * rows * rows),
        name="scatter_out",
    )(q, k, v, wo, x, gain)


def mlp(b, w_gate, w_up, w_down, h):
    (_, half, d), f = b.shape, w_gate.shape[1]
    both, n = 2 * half, CHIPS * 2
    tiles = f // GU

    def kernel(b_ref, wg_ref, wu_ref, wd_ref, h_ref, y_ref, all_ref, xs, wg, wu, hid, *rest):
        *rest, gsend, grecv, xsem, gsem, usem, osem, free = rest
        place = Place()
        place.hello()
        s = Scatter(place, hid, wd_ref, xs.at[0, pl.ds(both, both)], *rest)

        def land(piece):
            wave = [piece in w for w in WAVES].index(True)
            return xs.at[wave % 2, pl.ds((2 + WAVES[wave].index(piece)) * half, half)]

        g = Gather(place, b_ref, all_ref, gsend, grecv, land)

        def weights(u):
            at = pl.ds(pl.multiple_of(lax.rem(u, tiles) * GU, GU), GU)
            slot = lax.rem(u, 2)
            return (pltpu.make_async_copy(wg_ref.at[:, at], wg.at[slot], gsem.at[slot]),
                    pltpu.make_async_copy(wu_ref.at[:, at], wu.at[slot], usem.at[slot]))

        def fetch(wave):
            return [pltpu.make_async_copy(g.piece(piece), xs.at[wave % 2, pl.ds(i * half, half)], xsem.at[wave % 2, i])
                    for i, piece in enumerate(WAVES[wave])]

        def start(copies):
            for c in copies:
                c.start()

        def wait(copies):
            for c in copies:
                c.wait()

        def near(wave):
            for p in WAVES[wave]:
                g.arrive(p)
            if wave == 1:
                g.onward(LO).start()
                g.onward(HI).start()
                g.to_next(HI).start()
                g.to_previous(LO).start()
            else:
                pl.semaphore_wait(free.at[wave % 2], 1)
            for p in WAVES[wave]:
                g.across(p).start()
            start(fetch(wave))

        def far(wave):
            for p in WAVES[wave]:
                g.arrive(p, True)

        start(weights(0))
        start(fetch(0))
        s.load(0).start()
        s.load(1).start()
        place.meet()
        g.to_next(LO).start()
        g.to_previous(HI).start()
        for piece in WAVES[0]:
            g.across(piece).start()
        far(0)

        def hidden(u, wave, slot):
            at = pl.ds(pl.multiple_of(lax.rem(u, tiles) * GU, GU), GU)
            two = lax.rem(u, 2)

            gate = jnp.dot(xs[slot], wg[two], preferred_element_type=jnp.float32)
            up = jnp.dot(xs[slot], wu[two], preferred_element_type=jnp.float32)
            hid[wave, :, at] = (jax.nn.silu(gate) * up).astype(jnp.bfloat16)

        def early(u, _):
            wave = lax.div(u, tiles)
            for k in (0, 1, 2):

                @pl.when(u == k * tiles)
                def _():
                    if k:
                        pl.semaphore_signal(free.at[(k - 1) % 2], inc=1, device_id={"tp": place.other}, device_id_type=MESH)
                        far(k)
                    wait(fetch(k))

                if k:

                    @pl.when(u == k * tiles - 1)
                    def _():
                        near(k)

            wait(weights(u))
            start(weights(u + 1))
            hidden(u, wave, lax.rem(wave, 2))

        lax.fori_loop(0, 3 * tiles, early, None)
        near(3)
        residual = pltpu.make_async_copy(h_ref, xs.at[0, pl.ds(0, both)], xsem.at[0, 0])
        residual.start()
        s.wave(0, 2)
        far(3)
        s.wave(1, 1)
        wait(fetch(3))

        def late(u, _):
            wait(weights(u))

            @pl.when(u < 4 * tiles - 1)
            def _():
                start(weights(u + 1))

            hidden(u, 3, 1)

        lax.fori_loop(3 * tiles, 4 * tiles, late, None)
        s.wave(2, 3)
        residual.wait()

        def final(t, parts):
            at = pl.ds(pl.multiple_of(t * TN, TN), TN)
            for side in (0, 1):
                here = pl.ds(side * half, half)
                xs[0, here, at] = (xs[0, here, at].astype(jnp.float32) + parts[side]).astype(jnp.bfloat16)

        s.wave(3, 0, final)
        give = pltpu.make_async_copy(xs.at[0, pl.ds(0, both)], y_ref, osem)
        give.start()
        give.wait()
        g.drain(ACROSS)
        s.drain()

    return pl.pallas_call(
        kernel,
        out_shape=[jax.ShapeDtypeStruct((both, d), jnp.bfloat16), jax.ShapeDtypeStruct((n, 2, half, d), jnp.bfloat16)],
        in_specs=[ANY] * 5,
        out_specs=[ANY] * 2,
        scratch_shapes=[
            pltpu.VMEM((2, 4 * half, d), jnp.bfloat16),
            pltpu.VMEM((2, d, GU), jnp.bfloat16),
            pltpu.VMEM((2, d, GU), jnp.bfloat16),
            pltpu.VMEM((4, 4 * half, f), jnp.bfloat16),
            *Scatter.scratch(half, f, d),
            pltpu.SemaphoreType.DMA((14,)),
            pltpu.SemaphoreType.DMA((14,)),
            pltpu.SemaphoreType.DMA((2, 2)),
            pltpu.SemaphoreType.DMA((2,)),
            pltpu.SemaphoreType.DMA((2,)),
            pltpu.SemaphoreType.DMA,
            pltpu.SemaphoreType.REGULAR((2,)),
        ],
        compiler_params=pltpu.CompilerParams(collective_id=2, has_side_effects=True, vmem_limit_bytes=MOST),
        cost_estimate=pl.CostEstimate(flops=6 * n * both * d * f, bytes_accessed=24 * d * f, transcendentals=n * both * f),
        name="mlp",
    )(b, w_gate, w_up, w_down, h)[0]


def solution(mesh):
    def step(x, gain_a, wq, wk, wv, wo, gain_m, w_gate, w_up, w_down):
        both = x.shape[0]
        rows = both * mesh.shape["tp"]
        q, k, v = gather_qkv(x, gain_a[None], wq, wk, wv, *turns(rows, both // 4, THETA))
        h, b = scatter_out(q, k, v, wo, x, gain_m[None])
        return mlp(b, w_gate, w_up, w_down, h)

    tokens, columns, rows_of = P(("dp", "tp"), None), P(None, "tp"), P("tp", None)
    return jax.shard_map(
        step,
        mesh=mesh,
        in_specs=(tokens, P(None), columns, columns, columns, rows_of, P(None), columns, columns, rows_of),
        out_specs=tokens,
        check_vma=False,
    )
```

```python
import functools

import jax
import jax.numpy as jnp
from jax import lax
from jax.experimental import pallas as pl
from jax.experimental.pallas import tpu as pltpu


from jax.sharding import PartitionSpec as P

VMEM = 56 * 2**20
MOST = 67_043_328
HIDDEN = -1e30
LOG2E = 1.4426950408889634
KEYS = 512

HEAD = 128
THETA = 10000
MESH = pl.DeviceIdType.MESH
CHIPS = 4
LO, HI = 0, 1
WAVES = (((0, LO), (0, HI)), ((-1, LO), (1, HI)), ((2, LO), (2, HI)), ((-1, HI), (1, LO)))
RING = (WAVES[1] + WAVES[3] + WAVES[2])
ACROSS = WAVES[0] + RING
GU = 256
TN = 512
ANY = pl.BlockSpec(memory_space=pl.ANY)
WHOLE = pl.BlockSpec(memory_space=pltpu.VMEM)


def normed(x, gain):
    wide = x.astype(jnp.float32)
    scale = lax.rsqrt(jnp.mean(wide * wide, -1, keepdims=True) + 1e-6)
    return (wide * scale * gain.astype(jnp.float32)).astype(jnp.bfloat16)


def turns(rows, fine, theta):
    half = HEAD // 2

    def both(places):
        angle = places.astype(jnp.float32)[:, None] * theta ** (-jnp.arange(half, dtype=jnp.float32) / half)
        return jnp.cos(angle), jnp.sin(angle)

    cos, sin = both(jnp.arange(rows // fine) * fine)
    coarse = jnp.stack([jnp.concatenate([cos, cos], -1), jnp.concatenate([sin, sin], -1)], 1)
    cos, sin = both(jnp.arange(fine))
    return coarse, jnp.stack([jnp.concatenate(t, -1) for t in ((cos, cos), (sin, sin), (-cos, cos), (-sin, sin))])


class Place:
    def __init__(self):
        me = lax.axis_index("tp")
        self.me, self.chip, self.core = me, lax.div(me, 2), lax.rem(me, 2)
        self.next, self.previous, self.other = self.device(1), self.device(-1), self.device(0, True)

    def device(self, away, across=False):
        return lax.rem(self.chip + (away + CHIPS), CHIPS) * 2 + (1 - self.core if across else self.core)

    def hello(self):
        for d in (self.next, self.previous, self.other):
            pl.semaphore_signal(pltpu.get_barrier_semaphore(), inc=1, device_id={"tp": d}, device_id_type=MESH)

    def meet(self):
        pl.semaphore_wait(pltpu.get_barrier_semaphore(), 3)


def remote(src, dst, send, recv, to):
    return pltpu.make_async_remote_copy(src_ref=src, dst_ref=dst, send_sem=send, recv_sem=recv, device_id={"tp": to}, device_id_type=MESH)


class Gather:
    def __init__(self, place, own, all_, send, recv, land=None):
        self.place, self.own, self.all, self.send, self.recv, self.land = place, own, all_, send, recv, land

    def to_next(self, half):
        i = RING.index((-1, half))
        return remote(self.own.at[half], self.all.at[self.place.me, half], self.send.at[half], self.recv.at[i], self.place.next)

    def to_previous(self, half):
        i = RING.index((1, half))
        return remote(self.own.at[half], self.all.at[self.place.me, half], self.send.at[2 + half], self.recv.at[i], self.place.previous)

    def onward(self, half):
        ref = self.all.at[self.place.device(-1 if half == LO else 1), half]
        to = self.place.next if half == LO else self.place.previous
        return remote(ref, ref, self.send.at[4 + half], self.recv.at[RING.index((2, half))], to)

    def across(self, piece):
        i = 6 + ACROSS.index(piece)
        away, half = piece
        dst = self.all.at[self.place.device(away), half]
        src = self.own.at[half] if away == 0 else dst
        return remote(src, self.land(piece) if self.land else dst, self.send.at[i], self.recv.at[i], self.place.other)

    def arrive(self, piece, across=False):
        away, half = piece
        ref = self.land(piece) if across and self.land else self.all.at[self.place.device(away, across), half]
        i = 6 + ACROSS.index(piece) if across else RING.index(piece)
        remote(ref, ref, self.send.at[i], self.recv.at[i], self.place.other).wait_recv()

    def piece(self, piece, across=False):
        away, half = piece
        return self.own.at[half] if away == 0 and not across else self.all.at[self.place.device(away, across), half]

    def drain(self, pieces):
        for half in (LO, HI):
            self.to_next(half).wait_send()
            self.to_previous(half).wait_send()
            if (2, half) in pieces:
                self.onward(half).wait_send()
        for piece in pieces:
            self.across(piece).wait_send()


def normalize(ref, to, first, count, gain_ref):
    many = 32

    def some(i, _):
        here = pl.ds(pl.multiple_of(first + i * many, many), many)
        to[here, :] = normed(ref[here, :], gain_ref[...])

    lax.fori_loop(0, count // many, some, None)


def gather_qkv(x, gain, wq, wk, wv, coarse, fine):
    both, d = x.shape
    half, quarter = both // 2, both // 4
    n = CHIPS * 2
    rows, heads = n * both, wq.shape[1] // HEAD
    order = (0, 1, 3, 2)

    def kernel(x_ref, gain_ref, wq_ref, wk_ref, wv_ref, coarse_ref, fine_ref, q_ref, k_ref, v_ref, all_ref, own_ref,
               w, xs, st, send, recv, psend, precv, wsem, xsem, osem):
        place = Place()
        place.hello()
        quarters = [pl.ds(i * quarter, quarter) for i in range(4)]
        given = [pltpu.make_async_copy(x_ref.at[quarters[i]], xs.at[quarters[i]], xsem.at[i]) for i in range(4)]
        kept = [pltpu.make_async_copy(xs.at[quarters[i]], own_ref.at[i // 2, i % 2], xsem.at[i]) for i in range(4)]
        loads = [
            pltpu.make_async_copy(wq_ref, w.at[:, pl.ds(0, heads * HEAD)], wsem.at[0]),
            pltpu.make_async_copy(wk_ref, w.at[:, pl.ds(heads * HEAD, HEAD)], wsem.at[1]),
            pltpu.make_async_copy(wv_ref, w.at[:, pl.ds((heads + 1) * HEAD, HEAD)], wsem.at[2]),
        ]
        for c in given:
            c.start()
        for i in range(4):
            given[i].wait()
            normalize(xs, xs, i * quarter, quarter, gain_ref)
            kept[i].start()
        place.meet()
        g = Gather(place, own_ref, all_ref, send, recv)
        for c in kept:
            c.wait()
        g.to_next(LO).start()
        g.to_previous(HI).start()
        for piece in WAVES[0]:
            g.across(piece).start()
        g.to_next(HI).start()
        g.to_previous(LO).start()
        for c in loads:
            c.start()
        for c in loads:
            c.wait()

        def parts(v):
            if v < 6:
                return [(p, v % 2 == 1, i) for p in WAVES[order[v // 2]] for i in (0, 1)]
            return [(p, across, v - 6) for across in (False, True) for p in WAVES[2]]

        def block(v, i):
            at = 0
            for s in range(8):
                (away, h), across, e = parts(s)[i]
                at = jnp.where(v == s, place.device(away, across) * 4 + h * 2 + e, at)
            return at

        def opposite(h, e, across):
            ref = all_ref.at[place.device(2), h, e]
            if across:
                return remote(ref, ref, psend.at[1, h, e], precv.at[1, h, e], place.other)
            ref = all_ref.at[place.device(-1 if h == LO else 1), h, e]
            return remote(ref, ref, psend.at[0, h, e], precv.at[0, h, e], place.next if h == LO else place.previous)

        def reached(h, e, across):
            ref = all_ref.at[place.device(2, across), h, e]
            k = 1 if across else 0
            remote(ref, ref, psend.at[k, h, e], precv.at[k, h, e], place.other).wait_recv()

        def outs(slot, v):
            r = []
            for i in range(4):
                here = quarters[i]
                to = pl.ds(pl.multiple_of(block(v, i) * quarter, quarter), quarter)
                r.append(pltpu.make_async_copy(st.at[slot, pl.ds(0, heads), here], q_ref.at[:, to], osem.at[slot, i, 0]))
                r.append(pltpu.make_async_copy(st.at[slot, heads, here], k_ref.at[0, to], osem.at[slot, i, 1]))
                r.append(pltpu.make_async_copy(st.at[slot, heads + 1, here], v_ref.at[0, to], osem.at[slot, i, 2]))
            return r

        def fetch(v, which):
            copies = []
            for i in which:
                piece, across, e = parts(v)[i]
                copies.append(pltpu.make_async_copy(g.piece(piece, across).at[e], xs.at[quarters[i]], xsem.at[i]))
            for c in copies:
                c.start()
            return copies

        def ready(v):
            wave = order[v // 2]
            if v >= 6:
                for h in (LO, HI):
                    reached(h, v - 6, False)
                    opposite(h, v - 6, True).start()
                copies = fetch(v, (0, 1))
                for h in (LO, HI):
                    reached(h, v - 6, True)
                copies += fetch(v, (2, 3))
            else:
                for p in WAVES[wave]:
                    g.arrive(p, v % 2 == 1)
                if v == 2:
                    for e in (0, 1):
                        for h in (LO, HI):
                            opposite(h, e, False).start()
                if v % 2 == 0:
                    for p in WAVES[wave]:
                        g.across(p).start()
                copies = fetch(v, range(4))
            for c in copies:
                c.wait()

        def step(v, _):
            for s in range(1, 8):
                pl.when(v == s)(functools.partial(ready, s))

            slot = lax.rem(v, 2)

            @pl.when(v >= 2)
            def _():
                for c in outs(slot, v - 2):
                    c.wait()

            def chunk(j, _):
                at = pl.multiple_of(j * 2 * HEAD, 2 * HEAD)
                t = jnp.dot(xs[...], w[:, pl.ds(at, 2 * HEAD)], preferred_element_type=jnp.float32).astype(jnp.bfloat16).astype(jnp.float32)
                for i in range(4):
                    a = coarse_ref[block(v, i)]
                    cos = a[:1] * fine_ref[0] - a[1:] * fine_ref[1]
                    sin = a[1:] * fine_ref[2] + a[:1] * fine_ref[3]
                    for e in (0, 1):
                        u = t[i * quarter : (i + 1) * quarter, e * HEAD : (e + 1) * HEAD]
                        st[slot, 2 * j + e, i * quarter : (i + 1) * quarter, :] = (u * cos + pltpu.roll(u, HEAD // 2, 1) * sin).astype(jnp.bfloat16)

            lax.fori_loop(0, (heads + 1) // 2, chunk, None)
            st[slot, heads + 1] = jnp.dot(xs[...], w[:, (heads + 1) * HEAD :], preferred_element_type=jnp.float32).astype(jnp.bfloat16)
            for c in outs(slot, v):
                c.start()

        lax.fori_loop(0, 2 * CHIPS, step, None)
        for slot in (0, 1):
            for c in outs(slot, 2 * CHIPS - 2 + slot):
                c.wait()
        g.drain(WAVES[0] + WAVES[1] + WAVES[3])
        for h in (LO, HI):
            for e in (0, 1):
                opposite(h, e, False).wait_send()
                opposite(h, e, True).wait_send()

    return pl.pallas_call(
        kernel,
        out_shape=[
            jax.ShapeDtypeStruct((heads, rows, HEAD), jnp.bfloat16),
            jax.ShapeDtypeStruct((1, rows, HEAD), jnp.bfloat16),
            jax.ShapeDtypeStruct((1, rows, HEAD), jnp.bfloat16),
            jax.ShapeDtypeStruct((n, 2, 2, quarter, d), jnp.bfloat16),
            jax.ShapeDtypeStruct((2, 2, quarter, d), jnp.bfloat16),
        ],
        in_specs=[ANY, WHOLE, ANY, ANY, ANY, WHOLE, WHOLE],
        out_specs=[ANY] * 5,
        scratch_shapes=[
            pltpu.VMEM((d, (heads + 2) * HEAD), jnp.bfloat16),
            pltpu.VMEM((both, d), jnp.bfloat16),
            pltpu.VMEM((2, heads + 2, both, HEAD), jnp.bfloat16),
            pltpu.SemaphoreType.DMA((14,)),
            pltpu.SemaphoreType.DMA((14,)),
            pltpu.SemaphoreType.DMA((2, 2, 2)),
            pltpu.SemaphoreType.DMA((2, 2, 2)),
            pltpu.SemaphoreType.DMA((3,)),
            pltpu.SemaphoreType.DMA((4,)),
            pltpu.SemaphoreType.DMA((2, 4, 3)),
        ],
        compiler_params=pltpu.CompilerParams(collective_id=0, has_side_effects=True, vmem_limit_bytes=VMEM),
        cost_estimate=pl.CostEstimate(flops=2 * rows * d * (heads + 2) * HEAD, bytes_accessed=2 * rows * d * 2, transcendentals=0),
        name="gather_qkv",
    )(x, gain, wq, wk, wv, coarse, fine)[:3]


class Scatter:
    def __init__(self, place, hid, right, out, wd, sent, came, mine, passed, wsem, asend, arecv, ssem, rsem, clear):
        self.place, self.hid, self.right, self.wd, self.sent, self.came, self.mine, self.out, self.passed = (
            place, hid, right, wd, sent, came, mine, out, passed)
        self.wsem, self.asend, self.arecv, self.ssem, self.rsem, self.clear = wsem, asend, arecv, ssem, rsem, clear
        self.tiles = right.shape[1] // TN
        self.half = sent.shape[1] // 2

    @staticmethod
    def scratch(half, k, d):
        tiles = d // TN
        return [
            pltpu.VMEM((3, k, TN), jnp.bfloat16),
            pltpu.VMEM((2, 2 * half, TN), jnp.bfloat16),
            pltpu.VMEM((6, 2 * half, TN), jnp.bfloat16),
            pltpu.VMEM((3, 2 * half, TN), jnp.float32),
            pltpu.VMEM((2, 2, tiles, half, TN), jnp.bfloat16),
            pltpu.SemaphoreType.DMA((3,)),
            pltpu.SemaphoreType.DMA((2,)),
            pltpu.SemaphoreType.DMA((6,)),
            pltpu.SemaphoreType.DMA((2, tiles)),
            pltpu.SemaphoreType.DMA((3, 2, tiles)),
            pltpu.SemaphoreType.REGULAR((2,)),
        ]

    def load(self, t):
        at = pl.multiple_of(lax.rem(t, self.tiles) * TN, TN)
        slot = lax.rem(t, 3)
        return pltpu.make_async_copy(self.right.at[:, pl.ds(at, TN)], self.wd.at[slot], self.wsem.at[slot])

    def swap(self, t):
        two, six = lax.rem(t, 2), lax.rem(t, 6)
        return remote(self.sent.at[two], self.came.at[six], self.asend.at[two], self.arecv.at[six], self.place.other)

    def leaving(self, side, t):
        return pl.ds(side * self.half, self.half), pl.ds(pl.multiple_of(t * TN, TN), TN)

    def passing(self, k, side, t):
        to = self.place.previous if side == 0 else self.place.next
        return remote(self.out.at[self.leaving(side, t)], self.passed.at[k % 2, side, t], self.ssem.at[side, t], self.rsem.at[k, side, t], to)

    def wave(self, turn, wave, final=None):
        half, tiles = self.half, self.tiles
        base = turn * tiles

        def finish(t):
            g = base + t
            self.swap(g).wait_recv()
            sums = self.mine[lax.rem(g, 3)] + self.came[lax.rem(g, 6)].astype(jnp.float32)
            parts = [sums[:half], sums[half:]]
            if wave == 1:
                for side in (0, 1):
                    self.passing(0, side, t).wait_recv()
                    parts[side] += self.passed[0, side, t].astype(jnp.float32)
            if final is not None:
                for side in (0, 1):
                    self.passing(1, side, t).wait_recv()
                    self.passing(2, 1 - side, t).wait_recv()
                    parts[side] += self.passed[1, side, t].astype(jnp.float32) + self.passed[0, 1 - side, t].astype(jnp.float32)
                final(t, parts)
                return
            for side in (0, 1):
                if turn > 0:
                    self.passing(turn - 1, side, t).wait_send()
                self.out[self.leaving(side, t)] = parts[side].astype(jnp.bfloat16)
                self.passing(turn, side, t).start()

        def step(t, _):
            g = base + t
            slot = lax.rem(g, 3)
            self.load(g).wait()

            @pl.when(g < 4 * tiles - 2)
            def _():
                self.load(g + 2).start()

            def free():
                self.swap(g - 2).wait_send()

            if turn > 0:
                free()
            else:
                pl.when(t >= 2)(free)
            for a in range(0, TN, GU):
                here = slice(a, a + GU)
                terms = jnp.dot(self.hid[min(wave, 2)], self.wd[slot, :, here], preferred_element_type=jnp.float32)
                self.mine[lax.rem(g, 3), :, here] = terms[: 2 * half]
                self.sent[lax.rem(g, 2), :, here] = terms[2 * half :].astype(jnp.bfloat16)
            self.swap(g).start()

            @pl.when(t > 1)
            def _():
                finish(t - 2)

        if turn == 2:
            for side in (0, 1):
                pl.semaphore_wait(self.clear.at[side], 1)
        lax.fori_loop(0, tiles, step, None)
        finish(tiles - 2)
        finish(tiles - 1)
        if turn == 1:
            for side, to in ((0, self.place.next), (1, self.place.previous)):
                pl.semaphore_signal(self.clear.at[side], inc=1, device_id={"tp": to}, device_id_type=MESH)

    def drain(self):
        for i in (2, 1):
            self.swap(4 * self.tiles - i).wait_send()

        def one(t, _):
            for side in (0, 1):
                self.passing(2, side, t).wait_send()

        lax.fori_loop(0, self.tiles, one, None)


def scatter_out(q, k, v, wo, x, gain):
    (heads, rows, _), (both, d) = q.shape, x.shape
    half, width, block = both // 2, wo.shape[0], min(KEYS, rows)
    cols = heads * half
    strips = ((0, 4 * HEAD), (4 * HEAD, cols))
    scale = HEAD**-0.5 * LOG2E

    def dot(a, b, ca, cb):
        return lax.dot_general(a, b, (((ca,), (cb,)), ((), ())), preferred_element_type=jnp.float32)

    def kernel(q_ref, k_ref, v_ref, wo_ref, x_ref, gain_ref, h_ref, b_ref, hid, xs, bs, leave, qs, ks, vs, vt, top, mix, gap, *rest):
        *rest, qsem, ksem, xsem, osem = rest
        place = Place()
        place.hello()
        s = Scatter(place, hid, wo_ref, leave, *rest)

        def token(wave, p):
            away, h = WAVES[wave][p % 2]
            return pl.multiple_of(place.device(away, p >= 2) * both + h * half, half)

        def queries(wave, p):
            return pltpu.make_async_copy(q_ref.at[:, pl.ds(token(wave, p), half)], qs.at[wave, p], qsem.at[wave, p])

        kv = [pltpu.make_async_copy(k_ref.at[0], ks, ksem.at[0]), pltpu.make_async_copy(v_ref.at[0], vs, ksem.at[1])]
        for c in kv:
            c.start()
        for wave in (2, 1, 3, 0):
            for p in range(4):
                queries(wave, p).start()
        residual = pltpu.make_async_copy(x_ref, xs, xsem)
        residual.start()
        s.load(0).start()
        s.load(1).start()
        gap[...] = lax.broadcasted_iota(jnp.int32, gap.shape, 0) - lax.rem(lax.broadcasted_iota(jnp.int32, gap.shape, 1), half)
        for c in kv:
            c.wait()
        for i in range(rows // block):
            here = slice(i * block, (i + 1) * block)
            vt[:HEAD, here] = vs[here, :].T
        vt[HEAD:, :] = jnp.ones((16, rows), jnp.bfloat16)
        place.meet()

        def attention(wave):
            def piece(p, _):
                first = 0
                for i in range(4):
                    first = jnp.where(p == i, token(wave, i), first)
                top[...] = jnp.full(top.shape, HIDDEN, jnp.float32)
                mix[...] = jnp.zeros(mix.shape, jnp.float32)

                def some(j, masked):
                    here = pl.ds(pl.multiple_of(j * block, block), block)
                    mine = qs[wave, p].reshape(cols, HEAD)
                    scores = [dot(ks[here, :], mine[a:z, :], 1, 1) for a, z in strips]
                    weights, keeps = [], []
                    for (a, z), t in zip(strips, scores):
                        if masked:
                            t = jnp.where(gap[:, a:z] <= first - j * block, t, 2 * HIDDEN)
                        old = top[:, a:z]
                        new = jnp.maximum(old, t.max(axis=0, keepdims=True))
                        top[:, a:z] = new
                        weights.append(jnp.exp2((t - new) * scale).astype(jnp.bfloat16))
                        keeps.append(jnp.exp2((old - new) * scale))
                    for (a, z), t, keep in zip(strips, weights, keeps):
                        mix[:, a:z] = mix[:, a:z] * keep + dot(vt[:, here], t, 1, 0)

                last = lax.div(first, block)
                lax.fori_loop(0, last, lambda j, _: some(j, False), None)
                some(last, True)
                done = (mix[:HEAD, :] * (1 / mix[HEAD : HEAD + 1, :])).T.astype(jnp.bfloat16)
                at = pl.ds(pl.multiple_of(p * half, half), half)
                for i in range(heads):
                    hid[min(wave, 2), at, i * HEAD : (i + 1) * HEAD] = done[i * half : (i + 1) * half, :]

            for p in range(4):
                queries(wave, p).wait()
            lax.fori_loop(0, 4, piece, None)

        def final(t, parts):
            at = pl.ds(pl.multiple_of(t * TN, TN), TN)
            for side in (0, 1):
                here = pl.ds(side * half, half)
                xs[here, at] = (xs[here, at].astype(jnp.float32) + parts[side]).astype(jnp.bfloat16)

        attention(2)
        s.wave(0, 2)
        attention(1)
        attention(3)
        s.wave(1, 1)
        attention(0)
        s.wave(2, 3)
        residual.wait()
        s.wave(3, 0, final)
        keep = pltpu.make_async_copy(xs, h_ref, xsem)
        keep.start()
        give = [pltpu.make_async_copy(bs.at[pl.ds(i * half, half)], b_ref.at[i], osem.at[i]) for i in (0, 1)]
        for i in (0, 1):
            normalize(xs, bs, i * half, half, gain_ref)
            give[i].start()
        for c in (keep, *give):
            c.wait()
        s.drain()

    return pl.pallas_call(
        kernel,
        out_shape=[jax.ShapeDtypeStruct((both, d), jnp.bfloat16), jax.ShapeDtypeStruct((2, half, d), jnp.bfloat16)],
        in_specs=[ANY] * 5 + [WHOLE],
        out_specs=[ANY] * 2,
        scratch_shapes=[
            pltpu.VMEM((3, 4 * half, width), jnp.bfloat16),
            pltpu.VMEM((both, d), jnp.bfloat16),
            pltpu.VMEM((both, d), jnp.bfloat16),
            pltpu.VMEM((both, d), jnp.bfloat16),
            pltpu.VMEM((4, 4, heads, half, HEAD), jnp.bfloat16),
            pltpu.VMEM((rows, HEAD), jnp.bfloat16),
            pltpu.VMEM((rows, HEAD), jnp.bfloat16),
            pltpu.VMEM((HEAD + 16, rows), jnp.bfloat16),
            pltpu.VMEM((1, cols), jnp.float32),
            pltpu.VMEM((HEAD + 16, cols), jnp.float32),
            pltpu.VMEM((block, cols), jnp.int32),
            *Scatter.scratch(half, width, d),
            pltpu.SemaphoreType.DMA((4, 4)),
            pltpu.SemaphoreType.DMA((2,)),
            pltpu.SemaphoreType.DMA,
            pltpu.SemaphoreType.DMA((2,)),
        ],
        compiler_params=pltpu.CompilerParams(collective_id=1, has_side_effects=True, vmem_limit_bytes=VMEM),
        cost_estimate=pl.CostEstimate(flops=2 * rows * d * width, bytes_accessed=8 * d * width, transcendentals=heads * rows * rows),
        name="scatter_out",
    )(q, k, v, wo, x, gain)


def mlp(b, w_gate, w_up, w_down, h):
    (_, half, d), f = b.shape, w_gate.shape[1]
    both, n = 2 * half, CHIPS * 2
    tiles = f // GU

    def kernel(b_ref, wg_ref, wu_ref, wd_ref, h_ref, y_ref, all_ref, xs, wg, wu, hid, *rest):
        *rest, gsend, grecv, xsem, gsem, usem, osem, free = rest
        place = Place()
        place.hello()
        s = Scatter(place, hid, wd_ref, xs.at[0, pl.ds(both, both)], *rest)

        def land(piece):
            wave = [piece in w for w in WAVES].index(True)
            return xs.at[wave % 2, pl.ds((2 + WAVES[wave].index(piece)) * half, half)]

        g = Gather(place, b_ref, all_ref, gsend, grecv, land)

        def weights(u):
            at = pl.ds(pl.multiple_of(lax.rem(u, tiles) * GU, GU), GU)
            slot = lax.rem(u, 2)
            return (pltpu.make_async_copy(wg_ref.at[:, at], wg.at[slot], gsem.at[slot]),
                    pltpu.make_async_copy(wu_ref.at[:, at], wu.at[slot], usem.at[slot]))

        def fetch(wave):
            return [pltpu.make_async_copy(g.piece(piece), xs.at[wave % 2, pl.ds(i * half, half)], xsem.at[wave % 2, i])
                    for i, piece in enumerate(WAVES[wave])]

        def start(copies):
            for c in copies:
                c.start()

        def wait(copies):
            for c in copies:
                c.wait()

        def near(wave):
            for p in WAVES[wave]:
                g.arrive(p)
            if wave == 1:
                g.onward(LO).start()
                g.onward(HI).start()
                g.to_next(HI).start()
                g.to_previous(LO).start()
            else:
                pl.semaphore_wait(free.at[wave % 2], 1)
            for p in WAVES[wave]:
                g.across(p).start()
            start(fetch(wave))

        def far(wave):
            for p in WAVES[wave]:
                g.arrive(p, True)

        start(weights(0))
        start(fetch(0))
        s.load(0).start()
        s.load(1).start()
        place.meet()
        g.to_next(LO).start()
        g.to_previous(HI).start()
        for piece in WAVES[0]:
            g.across(piece).start()
        far(0)

        def hidden(u, wave, slot):
            at = pl.ds(pl.multiple_of(lax.rem(u, tiles) * GU, GU), GU)
            two = lax.rem(u, 2)

            gate = jnp.dot(xs[slot], wg[two], preferred_element_type=jnp.float32)
            up = jnp.dot(xs[slot], wu[two], preferred_element_type=jnp.float32)
            hid[jnp.minimum(wave, 2), :, at] = (jax.nn.silu(gate) * up).astype(jnp.bfloat16)

        def early(u, _):
            wave = lax.div(u, tiles)
            for k in (0, 1, 2):

                @pl.when(u == k * tiles)
                def _():
                    if k:
                        pl.semaphore_signal(free.at[(k - 1) % 2], inc=1, device_id={"tp": place.other}, device_id_type=MESH)
                        far(k)
                    wait(fetch(k))

                if k:

                    @pl.when(u == k * tiles - 1)
                    def _():
                        near(k)

            wait(weights(u))
            start(weights(u + 1))
            hidden(u, wave, lax.rem(wave, 2))

        lax.fori_loop(0, 3 * tiles, early, None)
        near(3)
        residual = pltpu.make_async_copy(h_ref, xs.at[0, pl.ds(0, both)], xsem.at[0, 0])
        residual.start()
        s.wave(0, 2)
        far(3)
        s.wave(1, 1)
        wait(fetch(3))

        def late(u, _):
            wait(weights(u))

            @pl.when(u < 4 * tiles - 1)
            def _():
                start(weights(u + 1))

            hidden(u, 3, 1)

        lax.fori_loop(3 * tiles, 4 * tiles, late, None)
        s.wave(2, 3)
        residual.wait()

        def final(t, parts):
            at = pl.ds(pl.multiple_of(t * TN, TN), TN)
            for side in (0, 1):
                here = pl.ds(side * half, half)
                xs[0, here, at] = (xs[0, here, at].astype(jnp.float32) + parts[side]).astype(jnp.bfloat16)

        s.wave(3, 0, final)
        give = pltpu.make_async_copy(xs.at[0, pl.ds(0, both)], y_ref, osem)
        give.start()
        give.wait()
        g.drain(ACROSS)
        s.drain()

    return pl.pallas_call(
        kernel,
        out_shape=[jax.ShapeDtypeStruct((both, d), jnp.bfloat16), jax.ShapeDtypeStruct((n, 2, half, d), jnp.bfloat16)],
        in_specs=[ANY] * 5,
        out_specs=[ANY] * 2,
        scratch_shapes=[
            pltpu.VMEM((2, 4 * half, d), jnp.bfloat16),
            pltpu.VMEM((2, d, GU), jnp.bfloat16),
            pltpu.VMEM((2, d, GU), jnp.bfloat16),
            pltpu.VMEM((3, 4 * half, f), jnp.bfloat16),
            *Scatter.scratch(half, f, d),
            pltpu.SemaphoreType.DMA((14,)),
            pltpu.SemaphoreType.DMA((14,)),
            pltpu.SemaphoreType.DMA((2, 2)),
            pltpu.SemaphoreType.DMA((2,)),
            pltpu.SemaphoreType.DMA((2,)),
            pltpu.SemaphoreType.DMA,
            pltpu.SemaphoreType.REGULAR((2,)),
        ],
        compiler_params=pltpu.CompilerParams(collective_id=2, has_side_effects=True, vmem_limit_bytes=MOST),
        cost_estimate=pl.CostEstimate(flops=6 * n * both * d * f, bytes_accessed=24 * d * f, transcendentals=n * both * f),
        name="mlp",
    )(b, w_gate, w_up, w_down, h)[0]


def solution(mesh):
    def step(x, gain_a, wq, wk, wv, wo, gain_m, w_gate, w_up, w_down):
        both = x.shape[0]
        rows = both * mesh.shape["tp"]
        q, k, v = gather_qkv(x, gain_a[None], wq, wk, wv, *turns(rows, both // 4, THETA))
        h, b = scatter_out(q, k, v, wo, x, gain_m[None])
        return mlp(b, w_gate, w_up, w_down, h)

    tokens, columns, rows_of = P(("dp", "tp"), None), P(None, "tp"), P("tp", None)
    return jax.shard_map(
        step,
        mesh=mesh,
        in_specs=(tokens, P(None), columns, columns, columns, rows_of, P(None), columns, columns, rows_of),
        out_specs=tokens,
        check_vma=False,
    )
```
